256 devices in a mesh: dp: 16 (over x_hi, z), tensor: 16 (over y, x_lo, core).
Axes of the slice: x: 4 (x_hi: 2, x_lo: 2; x = x_hi * 2 + x_lo), y: 4, z: 8, core: 2. Of those that a mesh axis runs over, the one named last changes fastest.
Arguments:
- tokens: bfloat16 [32768, 4608], P(('dp', 'tensor')), parts along dimension 0, may hold values from -6 to 6
- pre_gain: float32 [4608], replicated, may hold values from 0.1 to 1.9
- query_weight: bfloat16 [4608, 4096], P(None, 'tensor'), as said below
- key_weight: bfloat16 [4608, 2048], P(None, 'tensor'), as said below
- value_weight: bfloat16 [4608, 2048], P(None, 'tensor'), may hold values from -0.09375 to 0.09375
- out_weight: bfloat16 [4096, 4608], P('tensor'), may hold values from -0.09375 to 0.09375
- post_gain: float32 [4608], replicated, may hold values from 0.1 to 1.9
Outputs:
- layer_out: bfloat16 [32768, 4608], P(('dp', 'tensor')), parts along dimension 0
The draws below stay inside these ranges and needn't reach their ends.
There are 16 independent parts, one for each index of `dp`. The reference program is written for one: setup_inputs(seed, part) draws one part's arguments, and reference() takes and returns one part's arrays. A program takes and returns all parts, laid end to end along the dimension named above; an argument that names none is the same for every part. Nothing has to cross between parts.
Inputs may be any that keep to these rules, and one draw needn't show every extreme that they name: `query_weight`: entries lie within 16 / sqrt(4608) of zero. `key_weight`: entries lie within 16 / sqrt(4608) of zero.
All inputs are finite; a program needn't handle non-finite values.
Results may differ from the reference program's by a relative error of at most 0.015.
Values may be sent and summed in bfloat16 or wider, within the bound.
No kernel may reach another device: no remote copies, remote signals or barrier semaphores. Data moves between devices by JAX's collectives and lax.ppermute only.
A program may use at most 192 MiB of HBM per device.

```python
import jax
import jax.numpy as jnp
from jax import lax

D = 4608
HEADS = 32
KV_HEADS = 16
HEAD_DIM = 128
SEQ_LEN = 128
SEQS = 16
TOKENS = 2048
N_TENSOR = 16


def strong_head(key):
    return jax.random.randint(jax.random.fold_in(key, 5), (), 0, HEADS)


def head_gains(key, count, forced):
    spread = jax.random.uniform(key, (count,), jnp.float32)
    spread = jnp.where(jnp.arange(count) == forced, 1.0, spread)
    return 0.5 * jnp.power(8.0, spread)


def scaled_weight(key, count, forced):
    gains = head_gains(jax.random.fold_in(key, 1), count, forced)
    entries = jnp.clip(jax.random.normal(jax.random.fold_in(key, 2), (D, count * HEAD_DIM), jnp.float32), -4.0, 4.0)
    column_gain = jnp.repeat(gains, HEAD_DIM)
    return (entries * column_gain[None, :] / jnp.sqrt(jnp.float32(D))).astype(jnp.bfloat16)


def draw_query_weight(key, part):
    forced = strong_head(key)
    return scaled_weight(jax.random.fold_in(key, 11), HEADS, forced)


def draw_key_weight(key, part):
    forced = strong_head(key) // (HEADS // KV_HEADS)
    return scaled_weight(jax.random.fold_in(key, 23), KV_HEADS, forced)


def levels(rng, extent, shards, low, high):
    gain = 1.0
    for axis_at, blocks in shards:
        draws = jax.random.uniform(jax.random.fold_in(jax.random.fold_in(rng, 6), axis_at), (blocks,), jnp.float32, low / len(shards), high / len(shards))
        gain = gain * jnp.repeat(jnp.exp(draws), extent[axis_at] // blocks).reshape((-1,) + (1,) * (len(extent) - 1 - axis_at))
    return gain


def scatter_about(stream_key, shape, scale, reach, shards=(), kind=jnp.bfloat16):
    level = levels(stream_key, shape, shards, -0.22, 0.18) if shards else 1.0
    result = jax.random.normal(stream_key, shape, jnp.float32) * scale * level
    return jnp.minimum(jnp.maximum(result, -reach), reach).astype(kind)


def setup_inputs(seed: int = 0, part: int = 0) -> dict:
    key_list = jax.random.split(jax.random.key(seed), 8)
    own_keys = jax.random.split(jax.random.fold_in(key_list[7], part), 8)
    tokens = scatter_about(own_keys[0], (TOKENS, D), 1.0, 6.0, ((0, 16),))
    pre_gain = jnp.clip(1.0 + 0.18 * jax.random.normal(key_list[1], (D,), jnp.float32), 0.1, 1.9)
    query_weight = draw_query_weight(jax.random.fold_in(key_list[7], 71), part)
    key_weight = draw_key_weight(jax.random.fold_in(key_list[7], 71), part)
    value_weight = scatter_about(key_list[4], (D, KV_HEADS * HEAD_DIM), D ** -0.5, 0.09375, ((1, 16),))
    out_weight = scatter_about(key_list[5], (HEADS * HEAD_DIM, D), (HEADS * HEAD_DIM) ** -0.5, 0.09375, ((0, 16),))
    post_gain = jnp.clip(1.0 + 0.18 * jax.random.normal(key_list[6], (D,), jnp.float32), 0.1, 1.9)
    return dict(tokens=tokens, pre_gain=pre_gain, query_weight=query_weight, key_weight=key_weight, value_weight=value_weight, out_weight=out_weight, post_gain=post_gain)


norm_epsilon = 1e-06
soft_cap = 50.0
query_scale = 1.0 / 12.0
rope_base = 10000.0

def rms_scale(vectors, scale_gain):
    mean_square = lax.optimization_barrier(jnp.mean(vectors * vectors, axis=-1, keepdims=True))
    return vectors * lax.rsqrt(mean_square + norm_epsilon) * scale_gain.astype(jnp.float32)

def rotate(vectors, positions):
    half_dim = vectors.shape[-1] // 2
    exponent = jnp.arange(half_dim, dtype=jnp.float32) / half_dim
    angles = positions.astype(jnp.float32)[:, None] * jnp.power(rope_base, -exponent)[None, :]
    cosine = jnp.cos(angles)[:, None, :]
    sine_part = jnp.sin(angles)[:, None, :]
    first_half = vectors[..., :half_dim]
    second_half = vectors[..., half_dim:]
    return jnp.concatenate([first_half * cosine - second_half * sine_part, second_half * cosine + first_half * sine_part], axis=-1)

def attend(query, keys, values, query_pos, key_pos):
    query_count = query.shape[0]
    key_count = keys.shape[0]
    key_heads = keys.shape[1] // HEAD_DIM
    groups = query.shape[1] // keys.shape[1]
    query_four = query.reshape(query_count, key_heads, groups, HEAD_DIM).astype(jnp.float32)
    key_three = keys.reshape(key_count, key_heads, HEAD_DIM).astype(jnp.float32)
    value_three = values.reshape(key_count, key_heads, HEAD_DIM).astype(jnp.float32)
    raw_scores = jnp.einsum('qhgd,khd->hgqk', query_four, key_three, precision=lax.Precision.HIGHEST)
    capped = soft_cap * jnp.tanh(raw_scores * query_scale / soft_cap)
    allowed = jnp.logical_and(key_pos[None, :] <= query_pos[:, None], key_pos[None, :] // SEQ_LEN == query_pos[:, None] // SEQ_LEN)
    weights = jnp.where(allowed[None, None], jnp.exp(capped), 0.0)
    probability = (weights / lax.optimization_barrier(jnp.sum(weights, axis=-1, keepdims=True))).astype(jnp.bfloat16)
    mixed = jnp.einsum('hgqk,khd->qhgd', probability.astype(jnp.float32), value_three, precision=lax.Precision.HIGHEST)
    return mixed.astype(jnp.bfloat16).reshape(query_count, -1)

def reference(tokens, pre_gain, query_weight, key_weight, value_weight, out_weight, post_gain):
    token_count = tokens.shape[0]
    normed = rms_scale(tokens.astype(jnp.float32), pre_gain).astype(jnp.bfloat16)
    positions = jnp.arange(token_count, dtype=jnp.int32) % SEQ_LEN
    query = jnp.dot(normed, query_weight, preferred_element_type=jnp.float32)
    keys = jnp.dot(normed, key_weight, preferred_element_type=jnp.float32)
    values = jnp.dot(normed, value_weight, preferred_element_type=jnp.float32).astype(jnp.bfloat16)
    query = rotate(query.reshape(token_count, HEADS, HEAD_DIM), positions).reshape(token_count, HEADS * HEAD_DIM).astype(jnp.bfloat16)
    keys = rotate(keys.reshape(token_count, KV_HEADS, HEAD_DIM), positions).reshape(token_count, KV_HEADS * HEAD_DIM).astype(jnp.bfloat16)

    def one_sequence(seq_index):
        first_row = (seq_index * SEQ_LEN).astype(jnp.int32)
        token_pos = first_row + jnp.arange(SEQ_LEN, dtype=jnp.int32)
        return attend(lax.dynamic_slice_in_dim(query, first_row, SEQ_LEN, 0), lax.dynamic_slice_in_dim(keys, first_row, SEQ_LEN, 0), lax.dynamic_slice_in_dim(values, first_row, SEQ_LEN, 0), token_pos, token_pos)
    attended = lax.map(one_sequence, jnp.arange(SEQS, dtype=jnp.int32)).reshape(token_count, HEADS * HEAD_DIM)
    group_cols = HEADS * HEAD_DIM // N_TENSOR

    def add_group(group_index, running):
        first_col = (group_index * group_cols).astype(jnp.int32)
        group_term = jnp.dot(lax.dynamic_slice_in_dim(attended, first_col, group_cols, 1), lax.dynamic_slice_in_dim(out_weight, first_col, group_cols, 0), preferred_element_type=jnp.float32)
        rounded = lax.optimization_barrier(group_term.astype(jnp.bfloat16))
        return running + rounded.astype(jnp.float32)
    mixed = lax.fori_loop(0, N_TENSOR, add_group, jnp.zeros((token_count, D), jnp.float32))
    branch = rms_scale(mixed, post_gain)
    return (tokens.astype(jnp.float32) + branch).astype(jnp.bfloat16)
```

```python
import functools

import jax
import jax.numpy as jnp
from jax import lax
from jax.experimental import pallas as pl
from jax.experimental.pallas import tpu as pltpu
from jax.sharding import PartitionSpec as P

HEAD_DIM = 128
SEQ = 128
HALF = SEQ // 2
D = 4608
KT = 768
AX = ("dp", "tensor")

norm_epsilon = 1e-06
soft_cap = 50.0
query_scale = 1.0 / 12.0
rope_base = 10000.0


def place(x, y, z, core):
    x_hi, x_lo = divmod(x % 4, 2)
    return (x_hi * 8 + z) * 16 + ((y % 4) * 2 + x_lo) * 2 + core


def shift(value, dx=0, dy=0, swap=False):
    pairs = [
        (place(x, y, z, c), place(x + dx, y + dy, z, 1 - c if swap else c))
        for x in range(4)
        for y in range(4)
        for z in range(8)
        for c in range(2)
    ]
    return lax.ppermute(value, AX, pairs)


def rms_scale(vectors, gain):
    mean_square = jnp.mean(vectors * vectors, axis=-1, keepdims=True)
    return vectors * lax.rsqrt(mean_square + norm_epsilon) * gain


def rope_tables():
    half = HEAD_DIM // 2
    exponent = jnp.arange(half, dtype=jnp.float32) / half
    positions = jnp.arange(SEQ, dtype=jnp.float32)
    angles = positions[:, None] * jnp.power(rope_base, -exponent)[None, :]
    cosine, sine = jnp.cos(angles), jnp.sin(angles)
    return jnp.concatenate([cosine, cosine], axis=1), jnp.concatenate([-sine, sine], axis=1)


def attend_kernel(x0, xm, xp, x2a, x2b, wq, wk, wv, cos_ref, sin_ref, out_ref, acc_ref):
    step = pl.program_id(0)
    x = jnp.concatenate([x0[...], xm[...], xp[...], x2a[...], x2b[...]], axis=0)
    w = jnp.concatenate([wq[...], wk[...], wv[...]], axis=1)
    part = jnp.dot(x, w, preferred_element_type=jnp.float32)

    @pl.when(step == 0)
    def _():
        acc_ref[...] = part

    @pl.when(step > 0)
    def _():
        acc_ref[...] += part

    @pl.when(step == pl.num_programs(0) - 1)
    def _():
        cosine, sine = cos_ref[...], sin_ref[...]
        row = lax.broadcasted_iota(jnp.int32, (SEQ, SEQ), 0)
        col = lax.broadcasted_iota(jnp.int32, (SEQ, SEQ), 1)
        allowed = col <= row
        allowed = jnp.concatenate([allowed, allowed], axis=0)

        def rope(v):
            return (v * cosine + pltpu.roll(v, HEAD_DIM // 2, 1) * sine).astype(jnp.bfloat16)

        for s in range(4):
            rows = slice(s * SEQ, (s + 1) * SEQ)
            query = jnp.concatenate([rope(acc_ref[rows, 0:128]), rope(acc_ref[rows, 128:256])], axis=0)
            keys = rope(acc_ref[rows, 256:384])
            values = acc_ref[rows, 384:512].astype(jnp.bfloat16)
            raw = lax.dot_general(query, keys, (((1,), (1,)), ((), ())), preferred_element_type=jnp.float32)
            capped = soft_cap * jnp.tanh(raw * (query_scale / soft_cap))
            weights = jnp.where(allowed, jnp.exp(capped), 0.0)
            total = jnp.sum(weights, axis=-1, keepdims=True)
            probability = (weights * (1.0 / total)).astype(jnp.bfloat16)
            mixed = jnp.dot(probability, values, preferred_element_type=jnp.float32).astype(jnp.bfloat16)
            out_ref[rows, 0:128] = mixed[0:SEQ]
            out_ref[rows, 128:256] = mixed[SEQ:]


def attend(xs, wq, wk, wv, tables, name):
    column = lambda k: (0, k)
    row = lambda k: (k, 0)
    fixed = lambda k: (0, 0)
    return pl.pallas_call(
        attend_kernel,
        grid=(D // KT,),
        in_specs=[pl.BlockSpec((SEQ, KT), column)] * 3
        + [pl.BlockSpec((HALF, KT), column)] * 2
        + [pl.BlockSpec((KT, 256), row), pl.BlockSpec((KT, 128), row), pl.BlockSpec((KT, 128), row)]
        + [pl.BlockSpec((SEQ, HEAD_DIM), fixed)] * 2,
        out_specs=pl.BlockSpec((512, 256), fixed),
        out_shape=jax.ShapeDtypeStruct((512, 256), jnp.bfloat16),
        scratch_shapes=[pltpu.VMEM((512, 512), jnp.float32)],
        compiler_params=pltpu.CompilerParams(vmem_limit_bytes=24 << 20),
        cost_estimate=pl.CostEstimate(
            flops=2 * 512 * D * 512, bytes_accessed=2 * D * 1024, transcendentals=0
        ),
        name=name,
    )(*xs, wq, wk, wv, *tables)


def project_kernel(a0, a1, a2, a3, w0, w1, w2t, w2b, w3t, w3b, p0, p1, pm, p2a, p2b):
    total = jnp.dot(a0[...], w0[...], preferred_element_type=jnp.float32)
    total += jnp.dot(a1[...], w1[...], preferred_element_type=jnp.float32)
    w2 = jnp.concatenate([w2t[...], w2b[...]], axis=0)
    w3 = jnp.concatenate([w3t[...], w3b[...]], axis=0)
    total += jnp.dot(a2[...], w2, preferred_element_type=jnp.float32)
    total += jnp.dot(a3[...], w3, preferred_element_type=jnp.float32)
    result = total.astype(jnp.bfloat16)
    p0[...] = result[0:128]
    pm[...] = result[128:256]
    p1[...] = result[256:384]
    p2a[...] = result[384:448]
    p2b[...] = result[448:512]


def project(attended, whole, parts, chunk, columns, name):
    block = 384
    steps = columns // block
    first = chunk * steps
    fixed = lambda j: (0, 0)
    return pl.pallas_call(
        project_kernel,
        grid=(steps,),
        in_specs=[pl.BlockSpec((512, 256), fixed)] * 4
        + [pl.BlockSpec((256, block), lambda j: (0, first + j))] * 2
        + [pl.BlockSpec((128, block), lambda j: (0, j))] * 4,
        out_specs=[pl.BlockSpec((SEQ, block), lambda j: (0, j))] * 3
        + [pl.BlockSpec((HALF, block), lambda j: (0, j))] * 2,
        out_shape=[jax.ShapeDtypeStruct((SEQ, columns), jnp.bfloat16)] * 3
        + [jax.ShapeDtypeStruct((HALF, columns), jnp.bfloat16)] * 2,
        compiler_params=pltpu.CompilerParams(vmem_limit_bytes=24 << 20),
        cost_estimate=pl.CostEstimate(
            flops=2 * 512 * 1024 * columns, bytes_accessed=2 * columns * 1536, transcendentals=0
        ),
        name=name,
    )(*attended, *whole, *parts)


def body(tokens, pre_gain, query_weight, key_weight, value_weight, out_weight, post_gain):
    chunks = 2
    columns = D // chunks
    normed = rms_scale(tokens.astype(jnp.float32), pre_gain).astype(jnp.bfloat16)
    tables = rope_tables()

    from_below = shift(normed, dy=1)
    from_above = shift(normed, dy=-1)
    far_a = shift(from_below[:HALF], dy=1)
    far_b = shift(from_above[HALF:], dy=-1)
    xs = (normed, from_below, from_above, far_a, far_b)

    own = (query_weight, key_weight, value_weight)
    partner = tuple(shift(w, swap=True) for w in own)
    partner_out = shift(out_weight, swap=True)
    across = (
        shift(query_weight, dx=1),
        shift(key_weight, dx=-1),
        shift(value_weight, dx=-1),
    )
    across_partner = tuple(shift(w, swap=True) for w in across)
    out_parts = []
    for chunk in range(chunks):
        cols = slice(chunk * columns, (chunk + 1) * columns)
        top = shift(out_weight[:128, cols], dx=1)
        bottom = shift(out_weight[128:, cols], dx=-1)
        out_parts.append((top, bottom, shift(top, swap=True), shift(bottom, swap=True)))

    attended = [
        attend(xs, *weights, tables, f"attend{i}")
        for i, weights in enumerate((own, partner, across, across_partner))
    ]

    sums = []
    for chunk in range(chunks):
        p0, p1, pm, p2a, p2b = project(
            attended, (out_weight, partner_out), out_parts[chunk], chunk, columns, f"project{chunk}"
        )
        via_above = shift(p2a, dy=1)
        via_below = shift(p2b, dy=-1)
        up = jnp.concatenate(
            [(p1[:HALF].astype(jnp.float32) + via_above.astype(jnp.float32)).astype(jnp.bfloat16), p1[HALF:]], axis=0
        )
        down = jnp.concatenate(
            [pm[:HALF], (pm[HALF:].astype(jnp.float32) + via_below.astype(jnp.float32)).astype(jnp.bfloat16)], axis=0
        )
        got_below = shift(up, dy=1)
        got_above = shift(down, dy=-1)
        sums.append(
            p0.astype(jnp.float32) + got_below.astype(jnp.float32) + got_above.astype(jnp.float32)
        )
    mixed = jnp.concatenate(sums, axis=1)
    branch = rms_scale(mixed, post_gain)
    return (tokens.astype(jnp.float32) + branch).astype(jnp.bfloat16)


def solution(mesh):
    return jax.shard_map(
        body,
        mesh=mesh,
        in_specs=(
            P(("dp", "tensor"), None),
            P(),
            P(None, "tensor"),
            P(None, "tensor"),
            P(None, "tensor"),
            P("tensor", None),
            P(),
        ),
        out_specs=P(("dp", "tensor"), None),
        check_vma=False,
    )
```

```python
import jax
import jax.numpy as jnp
from jax import lax
from jax.experimental import pallas as pl
from jax.experimental.pallas import tpu as pltpu
from jax.sharding import PartitionSpec as P


HEAD_DIM = 128
SEQ = 128
HALF = SEQ // 2
D = 4608
MID = D // 2
KT = 768
BLOCK = 768
AX = ("dp", "tensor")

norm_epsilon = 1e-06
soft_cap = 50.0
query_scale = 1.0 / 12.0
rope_base = 10000.0


def place(x, y, z, core):
    x_hi, x_lo = divmod(x % 4, 2)
    return (x_hi * 8 + z % 8) * 16 + ((y % 4) * 2 + x_lo) * 2 + core


def shift(value, dx=0, dy=0, dz=0, swap=False):
    pairs = [
        (place(x, y, z, c), place(x + dx, y + dy, z + dz, 1 - c if swap else c))
        for x in range(4)
        for y in range(4)
        for z in range(8)
        for c in range(2)
    ]
    return lax.ppermute(value, AX, pairs)


def norm_kernel(x_ref, gain_ref, a_ref, b_ref):
    gain = gain_ref[...]
    for base, out_ref in ((0, a_ref), (HALF, b_ref)):

        @pl.loop(0, HALF // 16)
        def _(i, base=base, out_ref=out_ref):
            at = pl.multiple_of(i * 16, 16)
            x = x_ref[pl.ds(base + at, 16), :].astype(jnp.float32)
            square = jnp.sum(x * x, axis=-1, keepdims=True)
            scale = lax.rsqrt(square * (1.0 / D) + norm_epsilon)
            out_ref[pl.ds(at, 16), :] = (x * scale * gain).astype(jnp.bfloat16)


def norm(tokens, gain):
    return pl.pallas_call(
        norm_kernel,
        in_specs=[pl.BlockSpec(memory_space=pltpu.VMEM)] * 2,
        out_specs=[pl.BlockSpec(memory_space=pltpu.VMEM)] * 2,
        out_shape=[jax.ShapeDtypeStruct((HALF, D), jnp.bfloat16)] * 2,
        compiler_params=pltpu.CompilerParams(vmem_limit_bytes=16 << 20),
        cost_estimate=pl.CostEstimate(flops=4 * SEQ * D, bytes_accessed=4 * SEQ * D, transcendentals=0),
        name="norm",
    )(tokens, gain)


def finish_kernel(x_ref, gain_ref, p0, below_a, below_b, above_a, above_b, out_ref):
    rows = out_ref.shape[1]
    here = pl.ds(pl.multiple_of(pl.program_id(0) * rows, rows), rows)
    for half, below, above in ((0, below_a, above_a), (1, below_b, above_b)):
        mixed = [
            p0[side, half, here].astype(jnp.float32)
            + below[side, here].astype(jnp.float32)
            + above[side, here].astype(jnp.float32)
            for side in range(2)
        ]
        square = sum(jnp.sum(m * m, axis=-1, keepdims=True) for m in mixed)
        scale = lax.rsqrt(square * (1.0 / D) + norm_epsilon)
        for side in range(2):
            cols = slice(side * MID, (side + 1) * MID)
            branch = mixed[side] * scale * gain_ref[:, cols]
            out_ref[half, :, cols] = (x_ref[half, here, cols].astype(jnp.float32) + branch).astype(jnp.bfloat16)


def finish(tokens, gain, p0, *pieces):
    rows = 16
    vmem = pl.BlockSpec(memory_space=pltpu.VMEM)
    out = pl.pallas_call(
        finish_kernel,
        grid=(HALF // rows,),
        in_specs=[vmem] * 7,
        out_specs=pl.BlockSpec((2, rows, D), lambda i: (0, i, 0)),
        out_shape=jax.ShapeDtypeStruct((2, HALF, D), jnp.bfloat16),
        compiler_params=pltpu.CompilerParams(vmem_limit_bytes=12 << 20),
        cost_estimate=pl.CostEstimate(flops=8 * SEQ * D, bytes_accessed=10 * SEQ * D, transcendentals=0),
        name="finish",
    )(tokens.reshape(2, HALF, D), gain, p0.reshape(2, 2, HALF, MID), *pieces)
    return out.reshape(SEQ, D)


def rope_tables():
    half = HEAD_DIM // 2
    exponent = jnp.arange(half, dtype=jnp.float32) / half
    positions = jnp.arange(SEQ, dtype=jnp.float32)
    angles = positions[:, None] * jnp.power(rope_base, -exponent)[None, :]
    cosine, sine = jnp.cos(angles), jnp.sin(angles)
    return jnp.concatenate([cosine, cosine], axis=1), jnp.concatenate([-sine, sine], axis=1)


def make_attend_kernel(pieces, arrays, tops, bottoms):
    def kernel(flag, cos_ref, sin_ref, *refs):
        xs, refs = refs[:pieces], refs[pieces:]
        ws, (out_ref, acc_ref) = refs[:arrays], refs[arrays:]
        acc_ref[...] = jnp.zeros_like(acc_ref)

        @pl.loop(0, MID // KT)
        def _(step):
            at = pl.multiple_of(step * KT, KT)
            for base, parts in ((0, tops), (MID, bottoms)):
                x = jnp.concatenate([r[:, pl.ds(base + at, KT)] for r in xs], axis=0)
                w = jnp.concatenate(
                    [
                        ws[n][pl.ds(base + at, KT), :] if lead is None else ws[n][lead, pl.ds(at, KT), :]
                        for n, lead in parts
                    ],
                    axis=1,
                )
                acc_ref[...] += jnp.dot(x, w, preferred_element_type=jnp.float32)

        same = flag[0] == 0
        cosine, sine = cos_ref[...], sin_ref[...]
        row = lax.broadcasted_iota(jnp.int32, (SEQ, SEQ), 0)
        col = lax.broadcasted_iota(jnp.int32, (SEQ, SEQ), 1)
        allowed = col <= row
        allowed = jnp.concatenate([allowed, allowed], axis=0)

        def rope(v):
            return (v * cosine + pltpu.roll(v, HEAD_DIM // 2, 1) * sine).astype(jnp.bfloat16)

        for s in range(acc_ref.shape[0] // SEQ):
            rows = slice(s * SEQ, (s + 1) * SEQ)
            pair = lambda at: (acc_ref[rows, at : at + 128], acc_ref[rows, at + 128 : at + 256])
            first, second = pair(0)
            third, fourth = pair(256)
            keys = rope(jnp.where(same, third, fourth))
            values = jnp.where(same, fourth, third).astype(jnp.bfloat16)
            query = jnp.concatenate(
                [rope(jnp.where(same, first, second)), rope(jnp.where(same, second, first))], axis=0
            )
            raw = lax.dot_general(query, keys, (((1,), (1,)), ((), ())), preferred_element_type=jnp.float32)
            capped = soft_cap * jnp.tanh(raw * (query_scale / soft_cap))
            weights = jnp.where(allowed, jnp.exp(capped), 0.0)
            total = jnp.sum(weights, axis=-1, keepdims=True)
            probability = (weights * (1.0 / total)).astype(jnp.bfloat16)
            mixed = jnp.dot(probability, values, preferred_element_type=jnp.float32).astype(jnp.bfloat16)
            out_ref[rows, 0:128] = mixed[0:SEQ]
            out_ref[rows, 128:256] = mixed[SEQ:]

    return kernel


def attend(xs, arrays, tops, bottoms, flag, tables):
    rows = sum(x.shape[0] for x in xs)
    vmem = pl.BlockSpec(memory_space=pltpu.VMEM)
    return pl.pallas_call(
        make_attend_kernel(len(xs), len(arrays), tops, bottoms),
        in_specs=[pl.BlockSpec(memory_space=pltpu.SMEM)] + [vmem] * (2 + len(xs) + len(arrays)),
        out_specs=vmem,
        out_shape=jax.ShapeDtypeStruct((rows, 256), jnp.bfloat16),
        scratch_shapes=[pltpu.VMEM((rows, 512), jnp.float32)],
        compiler_params=pltpu.CompilerParams(vmem_limit_bytes=12 << 20),
        cost_estimate=pl.CostEstimate(
            flops=2 * rows * D * 512, bytes_accessed=2 * D * (rows + 512), transcendentals=0
        ),
    )(flag, *tables, *xs, *arrays)


def project_kernel(flag, *refs):
    a = jnp.concatenate([r[...] for r in refs[:4]], axis=1)
    whole, direct, shared, outs = refs[4:6], refs[6:10], refs[10:14], refs[14:]
    same = flag[0] == 0

    @pl.loop(0, MID // BLOCK)
    def _(step):
        at = pl.multiple_of(step * BLOCK, BLOCK)
        for side in range(2):
            rows = [r[:, pl.ds(side * MID + at, BLOCK)] for r in whole]
            if side == 0:
                rows += [r[:, pl.ds(at, BLOCK)] for r in direct]
            else:
                for over_x, over_z in (shared[:2], shared[2:]):
                    for first, second in ((over_x, over_z), (over_z, over_x)):
                        rows += [
                            jnp.where(same, first[half, :, pl.ds(at, BLOCK)], second[half, :, pl.ds(at, BLOCK)])
                            for half in range(2)
                        ]
            w = jnp.concatenate(rows, axis=0)
            result = jnp.dot(a, w, preferred_element_type=jnp.float32).astype(jnp.bfloat16)
            row = 0
            for ref in outs:
                ref[side, :, pl.ds(at, BLOCK)] = result[row : row + ref.shape[1]]
                row += ref.shape[1]


def project(flag, attended, whole, direct, shared, out_rows):
    rows = sum(out_rows)
    vmem = pl.BlockSpec(memory_space=pltpu.VMEM)
    return pl.pallas_call(
        project_kernel,
        in_specs=[pl.BlockSpec(memory_space=pltpu.SMEM)] + [vmem] * 14,
        out_specs=[vmem] * len(out_rows),
        out_shape=[jax.ShapeDtypeStruct((2, r, MID), jnp.bfloat16) for r in out_rows],
        compiler_params=pltpu.CompilerParams(vmem_limit_bytes=12 << 20),
        cost_estimate=pl.CostEstimate(
            flops=2 * rows * 1024 * D, bytes_accessed=2 * D * (1024 + rows), transcendentals=0
        ),
    )(flag, *attended, *whole, *direct, *shared)


def pack_kernel(*refs):
    for index, ref in enumerate(refs[:-1]):
        refs[-1][index] = ref[...]


def pack(pieces):
    vmem = pl.BlockSpec(memory_space=pltpu.VMEM)
    shape = (len(pieces), *pieces[0].shape)
    return pl.pallas_call(
        pack_kernel,
        in_specs=[vmem] * len(pieces),
        out_specs=vmem,
        out_shape=jax.ShapeDtypeStruct(shape, jnp.bfloat16),
        compiler_params=pltpu.CompilerParams(vmem_limit_bytes=4 << 20),
        cost_estimate=pl.CostEstimate(flops=1 << 20, bytes_accessed=1 << 20, transcendentals=0),
    )(*pieces)


def add(a, b):
    return (a.astype(jnp.float32) + b.astype(jnp.float32)).astype(jnp.bfloat16)


def block(tokens, pre_gain, query_weight, key_weight, value_weight, out_weight, post_gain):
    flag = lax.axis_index("dp") & 1
    even = flag == 0
    tables = rope_tables()
    tok_a, tok_b = norm(tokens, pre_gain.reshape(1, D))

    split = {
        "s": jnp.where(even, key_weight, value_weight),
        "h": jnp.where(even, query_weight[:, :128], query_weight[:, 128:]),
        "r": jnp.where(even, out_weight[:128, MID:], out_weight[128:, MID:]),
    }
    over_x, over_z = {}, {}
    for n, w in split.items():
        cut = w.shape[0] // 2
        over_x[n] = shift(w[:cut], dx=1), shift(w[cut:], dx=-1)
        over_z[n] = shift(over_x[n][0], dz=1), shift(over_x[n][1], dz=-1)
    wide_x = pack(over_x["s"] + over_x["h"])
    wide_z = pack(over_z["s"] + over_z["h"])
    across = (wide_x, wide_z), (shift(wide_x, swap=True), shift(wide_z, swap=True))
    left = shift(out_weight[:128, :MID], dx=1), shift(out_weight[128:, :MID], dx=-1)
    direct = (*left, shift(left[0], swap=True), shift(left[1], swap=True))
    right = pack(over_x["r"]), pack(over_z["r"])
    shared = (*right, shift(right[0], swap=True), shift(right[1], swap=True))

    own = (query_weight, key_weight, value_weight)
    partner = tuple(shift(w, swap=True) for w in own)
    partner_out = shift(out_weight, swap=True)

    up_a = shift(tok_a, dy=1)
    down_b = shift(tok_b, dy=-1)
    up_b = shift(tok_b, dy=1)
    down_a = shift(tok_a, dy=-1)
    near = (tok_a, tok_b, up_a, up_b, down_a, down_b)
    far = (shift(up_a, dy=1), shift(down_b, dy=-1))

    zero = jnp.zeros((1,), jnp.int32)
    flags = flag.astype(jnp.int32).reshape(1)
    plain = ((0, None), (1, None), (2, None))
    top, bottom = ((0, 2), (1, 2), (0, 0), (1, 0)), ((0, 3), (1, 3), (0, 1), (1, 1))
    owners = [(own, plain, plain, zero), (partner, plain, plain, zero)]
    owners += [(arrays, top, bottom, flags) for arrays in across]
    attend_near = [attend(near, *owner, tables) for owner in owners]
    attend_far = [attend(far, *owner, tables) for owner in owners]
    weights = ((out_weight, partner_out), direct, shared)

    far_a, far_b = project(flags, attend_far, *weights, (HALF, HALF))
    via_above = shift(far_a, dy=1)
    via_below = shift(far_b, dy=-1)
    p0, down_part_a, down_part_b, up_part_a, up_part_b = project(
        flags, attend_near, *weights, (SEQ, HALF, HALF, HALF, HALF)
    )
    below_b = shift(up_part_b, dy=1)
    above_a = shift(down_part_a, dy=-1)
    up_part_a = add(up_part_a, via_above)
    below_a = shift(up_part_a, dy=1)
    down_part_b = add(down_part_b, via_below)
    above_b = shift(down_part_b, dy=-1)
    return finish(tokens, post_gain.reshape(1, D), p0, below_a, below_b, above_a, above_b)


def solution(mesh):
    return jax.shard_map(
        block,
        mesh=mesh,
        in_specs=(
            P(("dp", "tensor"), None),
            P(),
            P(None, "tensor"),
            P(None, "tensor"),
            P(None, "tensor"),
            P("tensor", None),
            P(),
        ),
        out_specs=P(("dp", "tensor"), None),
        check_vma=False,
    )
```
